64 devices in a mesh: rep: 4 (over x, y), dp: 16 (over z, core).
Axes of the slice: x: 2, y: 2, z: 8, core: 2. Of those that a mesh axis runs over, the one named last changes fastest.
The devices are a block of a 4x4x8 slice.
Arguments:
- x: bfloat16 [64, 2048, 768], P(('rep', 'dp')), parts along dimension 0
- dy: bfloat16 [64, 2048, 768], P(('rep', 'dp')), parts along dimension 0
- w_gate: bfloat16 [2, 768, 1792], replicated
- w_up: bfloat16 [2, 768, 1792], replicated
- w_down: bfloat16 [2, 1792, 768], replicated
- m_w_gate: float32 [2, 768, 1792], replicated
- m_w_up: float32 [2, 768, 1792], replicated
- m_w_down: float32 [2, 1792, 768], replicated
- v_w_gate: float32 [2, 768, 1792], replicated
- v_w_up: float32 [2, 768, 1792], replicated
- v_w_down: float32 [2, 1792, 768], replicated
Outputs:
- output 1: bfloat16 [8, 768, 1792], P('rep'), parts along dimension 0
- output 2: bfloat16 [8, 768, 1792], P('rep'), parts along dimension 0
- output 3: bfloat16 [8, 1792, 768], P('rep'), parts along dimension 0
- output 4: float32 [8, 768, 1792], P('rep'), parts along dimension 0
- output 5: float32 [8, 768, 1792], P('rep'), parts along dimension 0
- output 6: float32 [8, 1792, 768], P('rep'), parts along dimension 0
- output 7: float32 [8, 768, 1792], P('rep'), parts along dimension 0
- output 8: float32 [8, 768, 1792], P('rep'), parts along dimension 0
- output 9: float32 [8, 1792, 768], P('rep'), parts along dimension 0
There are 4 independent parts. The reference program is written for one: setup_inputs(seed, part) draws one part's arguments, and reference() takes and returns one part's arrays. A program takes and returns all parts, laid end to end along the dimension named above; an argument that names none is the same for every part.
All inputs are finite; a program needn't handle non-finite values.
Results may differ from the reference program's by a relative error of at most 0.0224.
Values are sent between devices in bfloat16 or wider.
A program may use at most 768 MiB of HBM per device.

```python
import jax
import jax.numpy as jnp
from jax import lax

SEQUENCES = 16
TOKENS = 2048
D = 768
FF = 1792
LAYERS = 2
NAMES = ("w_gate", "w_up", "w_down")
SHAPES = {"w_gate": (LAYERS, D, FF), "w_up": (LAYERS, D, FF), "w_down": (LAYERS, FF, D)}


def bump(key, n, height):
    away = (jnp.arange(n, dtype=jnp.int32) - jax.random.randint(key, (), 0, n, jnp.int32)) % n
    return jnp.where(away < n // 8, height, 1.0)


def together(key, own, strength):
    shared = jax.random.normal(key, own.shape[1:], jnp.float32)
    return (own + strength * shared) * lax.rsqrt(1 + strength * strength)


def setup_inputs(seed: int = 0, part: int = 0) -> dict:
    kx, kdy, ka, kb, kz, kf, kh, kl, *keys = jax.random.split(jax.random.key(seed), 8 + 3 * len(NAMES))
    kx, kdy, ka, kb = (jax.random.fold_in(k, part) for k in (kx, kdy, ka, kb))
    kw, km, kv = (keys[i::3] for i in range(3))
    shape = (SEQUENCES, TOKENS, D)
    much_x, much_dy = jax.random.uniform(kz, (2,), jnp.float32, 0.0, 1.0)
    loud = 2.0 ** jax.random.uniform(jax.random.fold_in(kz, 1), (), jnp.float32, -1.0, 2.0)
    layers = 2.0 ** jax.random.uniform(kl, (LAYERS, 1, 1), jnp.float32, -1.0, 1.0)
    x = together(ka, jax.random.normal(kx, shape, jnp.float32), much_x) * bump(kf, D, 4.0)
    dy = together(kb, jax.random.normal(kdy, shape, jnp.float32), much_dy)
    drawn = {"x": x.astype(jnp.bfloat16), "dy": (loud * dy * (SEQUENCES * TOKENS) ** -0.5).astype(jnp.bfloat16)}
    for key, name in zip(kw, NAMES, strict=True):
        w = jax.random.normal(key, SHAPES[name], jnp.float32) * SHAPES[name][1] ** -0.5
        drawn[name] = (w * {"w_gate": 1.0, "w_up": bump(kh, FF, 4.0), "w_down": layers}[name]).astype(jnp.bfloat16)
    for key, name in zip(km, NAMES, strict=True):
        drawn[f"m_{name}"] = 0.1 * jax.random.normal(key, SHAPES[name], jnp.float32)
    for key, name in zip(kv, NAMES, strict=True):
        drawn[f"v_{name}"] = jax.random.uniform(key, SHAPES[name], jnp.float32, 0.005, 0.015)
    return drawn


def matmul(a, w):
    return jnp.dot(a, w, preferred_element_type=jnp.float32).astype(jnp.bfloat16)


def normed(h):
    wide = h.astype(jnp.float32)
    scale = lax.rsqrt(jnp.mean(wide**2, -1, keepdims=True) + 1e-6)
    return (wide * scale).astype(jnp.bfloat16)


def layer(h, w):
    a = normed(h)
    gate = jnp.dot(a, w["w_gate"], preferred_element_type=jnp.float32)
    up = jnp.dot(a, w["w_up"], preferred_element_type=jnp.float32)
    return h + matmul((jax.nn.silu(gate) * up).astype(jnp.bfloat16), w["w_down"])


def adamw(w, m, v, g):
    m = 0.9 * m + 0.1 * g
    v = 0.95 * v + 0.05 * g * g
    step = m * lax.rsqrt(v + 1e-8) + 0.1 * w
    return (w - 0.02 * step).astype(jnp.bfloat16), m, v


def clipped(gradients, sum_of_squares, count):
    factor = jnp.minimum(1.0, 0.5 * lax.rsqrt(sum_of_squares / count + 1e-30))
    return [g * factor for g in gradients]


def stack(weights, h):
    return lax.scan(lambda h, w: (layer(h, w), None), h, weights)[0]


def reference(x, dy, w_gate, w_up, w_down, m_w_gate, m_w_up, m_w_down, v_w_gate, v_w_up, v_w_down):
    weights = dict(zip(NAMES, (w_gate, w_up, w_down), strict=True))

    def take(so_far, sequence):
        h, by_y = sequence
        _, back = jax.vjp(lambda w: stack(w, h), weights)
        return jax.tree.map(lambda total, term: total + term.astype(jnp.float32), so_far, back(by_y)[0]), None

    none_yet = {name: jnp.zeros(w.shape, jnp.float32) for name, w in weights.items()}
    by_weights, _ = lax.scan(take, none_yet, (x, dy))
    gradients = [by_weights[name].astype(jnp.bfloat16).astype(jnp.float32) for name in NAMES]
    gradients = clipped(gradients, sum(jnp.sum(g * g) for g in gradients), sum(g.size for g in gradients))
    new = [
        adamw(w.astype(jnp.float32), m, v, g)
        for w, m, v, g in zip((w_gate, w_up, w_down), (m_w_gate, m_w_up, m_w_down), (v_w_gate, v_w_up, v_w_down), gradients, strict=True)
    ]
    return tuple(one[which] for which in range(3) for one in new)
```

```python
import functools

import jax
import jax.numpy as jnp
from jax import lax
from jax.experimental import pallas as pl
from jax.experimental.pallas import tpu as pltpu
from jax.sharding import PartitionSpec as P

BLOCK = 256
ROWS = 512
VMEM = 64 * 1024 * 1024 - 65536
F32, BF16 = jnp.float32, jnp.bfloat16


def dot(a, b):
    return jnp.dot(a, b, preferred_element_type=F32)


def sigmoid(x):
    return 0.5 * jnp.tanh(0.5 * x) + 0.5


def inverse_rms(wide):
    return lax.rsqrt(jnp.mean(wide * wide, -1, keepdims=True) + 1e-6)


def normed(h):
    wide = h.astype(F32)
    return (wide * inverse_rms(wide)).astype(BF16)


def row_loop(tokens, body):
    def step(i, _):
        body(pl.ds(pl.multiple_of(i * ROWS, ROWS), ROWS))
        return 0

    lax.fori_loop(0, tokens // ROWS, step, 0)


def forward_kernel(x, gate, up, down, out, a, total):
    tokens = x.shape[0]
    j = pl.program_id(0)

    @pl.when(j == 0)
    def _():
        def start(rows):
            a[rows, :] = normed(x[rows, :])
            total[rows, :] = jnp.zeros((ROWS, total.shape[1]), F32)

        row_loop(tokens, start)

    def rows_of(rows):
        g = dot(a[rows, :], gate[0])
        u = dot(a[rows, :], up[0])
        hidden = (g * sigmoid(g) * u).astype(BF16)
        total[rows, :] += dot(hidden, down[0])

    row_loop(tokens, rows_of)

    @pl.when(j == pl.num_programs(0) - 1)
    def _():
        def finish(rows):
            out[rows, :] = x[rows, :] + total[rows, :].astype(BF16)

        row_loop(tokens, finish)


def block_specs(layer, d):
    return [
        pl.BlockSpec((1, d, BLOCK), lambda j: (layer, 0, j)),
        pl.BlockSpec((1, d, BLOCK), lambda j: (layer, 0, j)),
        pl.BlockSpec((1, BLOCK, d), lambda j: (layer, j, 0)),
    ]


def forward(x, w_gate, w_up, w_down):
    tokens, d = x.shape
    blocks = w_gate.shape[2] // BLOCK
    whole = pl.BlockSpec((tokens, d), lambda j: (0, 0))
    return pl.pallas_call(
        forward_kernel,
        out_shape=jax.ShapeDtypeStruct((tokens, d), BF16),
        grid=(blocks,),
        in_specs=[whole] + block_specs(0, d),
        out_specs=whole,
        scratch_shapes=[pltpu.VMEM((tokens, d), BF16), pltpu.VMEM((tokens, d), F32)],
        compiler_params=pltpu.CompilerParams(vmem_limit_bytes=VMEM),
        name="forward",
    )(x, w_gate, w_up, w_down)


def backward_kernel(last, h, dy, gate, up, down, grads, *rest):
    if last:
        a, a_t, dy_t, both, hidden, down_t = rest
    else:
        dh, a, a_t, dy_t, both, hidden, down_t, w_t, total = rest
    tokens, d = h.shape
    j = pl.program_id(0)

    @pl.when(j == 0)
    def _():
        def start(rows):
            fresh = normed(h[rows, :])
            a[rows, :] = fresh
            a_t[:, rows] = fresh.T
            dy_t[:, rows] = dy[rows, :].T
            if not last:
                total[rows, :] = jnp.zeros((ROWS, d), F32)

        row_loop(tokens, start)

    down_t[...] = down[0].T
    if not last:
        w_t[0:BLOCK, :] = gate[0].T
        w_t[BLOCK:, :] = up[0].T

    def rows_of(rows):
        g = dot(a[rows, :], gate[0])
        u = dot(a[rows, :], up[0])
        dhid = dot(dy[rows, :], down_t[...]).astype(BF16).astype(F32)
        s = sigmoid(g)
        act = g * s
        hidden[rows, :] = (act * u).astype(BF16)
        both[rows, 0:BLOCK] = (dhid * u * (s + act * (1.0 - s))).astype(BF16)
        both[rows, BLOCK:] = (dhid * act).astype(BF16)
        if not last:
            total[rows, :] += dot(both[rows, :], w_t[...])

    row_loop(tokens, rows_of)
    grads[0, 0:d, :] = dot(a_t[...], both[:, 0:BLOCK]).astype(BF16)
    grads[0, d : 2 * d, :] = dot(a_t[...], both[:, BLOCK:]).astype(BF16)
    by_down = dot(dy_t[...], hidden[...])
    for t in range(d // BLOCK):
        grads[0, 2 * d + t * BLOCK : 2 * d + (t + 1) * BLOCK, :] = by_down[t * BLOCK : (t + 1) * BLOCK, :].T.astype(BF16)

    if not last:

        @pl.when(j == pl.num_programs(0) - 1)
        def _():
            def finish(rows):
                wide = h[rows, :].astype(F32)
                scale = inverse_rms(wide)
                by_a = total[rows, :].astype(BF16).astype(F32)
                by_scale = jnp.sum(by_a * wide, -1, keepdims=True)
                by_h = by_a * scale - wide * (scale * scale * scale * by_scale / d)
                dh[rows, :] = dy[rows, :] + by_h.astype(BF16)

            row_loop(tokens, finish)


def backward(layer, last, h, dy, w_gate, w_up, w_down):
    tokens, d = h.shape
    blocks = w_gate.shape[2] // BLOCK
    whole = pl.BlockSpec((tokens, d), lambda j: (0, 0))
    out_shape = [jax.ShapeDtypeStruct((blocks, 3 * d, BLOCK), BF16)]
    out_specs = [pl.BlockSpec((1, 3 * d, BLOCK), lambda j: (j, 0, 0))]
    scratch = [
        pltpu.VMEM((tokens, d), BF16),
        pltpu.VMEM((d, tokens), BF16),
        pltpu.VMEM((d, tokens), BF16),
        pltpu.VMEM((tokens, 2 * BLOCK), BF16),
        pltpu.VMEM((tokens, BLOCK), BF16),
        pltpu.VMEM((d, BLOCK), BF16),
    ]
    if not last:
        out_shape.append(jax.ShapeDtypeStruct((tokens, d), BF16))
        out_specs.append(whole)
        scratch += [pltpu.VMEM((2 * BLOCK, d), BF16), pltpu.VMEM((tokens, d), F32)]
    return pl.pallas_call(
        functools.partial(backward_kernel, last),
        out_shape=out_shape,
        grid=(blocks,),
        in_specs=[whole, whole] + block_specs(layer, d),
        out_specs=out_specs,
        scratch_shapes=scratch,
        compiler_params=pltpu.CompilerParams(vmem_limit_bytes=VMEM),
        name=f"backward_{layer}",
    )(h, dy, w_gate, w_up, w_down)


MESH = pl.DeviceIdType.MESH
LANES = 128
STREAMS = ((0, 4), (4, 3))


def put(grads, block, row, value):
    height = grads.shape[3]
    done = 0
    while done < value.shape[0]:
        piece, at = divmod(row + done, height)
        size = min(height - at, value.shape[0] - done)
        grads[block, piece // 2, piece % 2, at : at + size, :] = value[done : done + size, :]
        done += size


def exchange_kernel(group, h, dy, gate, up, down, other, out, norm_out, *scratch):
    (a, a_t, dy_t, both, hidden, down_t, own_grads, loc, sib0, sib1, ring00, ring01, ring10, ring11, final0, final1, norm, *sems) = scratch
    sib_send, sib_recv, loc_sem, rs_send, rs_recv, ag_send, ag_recv, pass_send, pass_recv, fin_sem, fin_send, fin_recv, norm_send, norm_recv = sems
    ring = ((ring00, ring01), (ring10, ring11))
    sib, final = (sib0, sib1), (final0, final1)
    tokens, d = h.shape
    blocks = own_grads.shape[0]
    chips = group // 2
    j = pl.program_id(0)
    me = lax.axis_index("dp")
    z, c = lax.div(me, 2), lax.rem(me, 2)
    sibling = me + 1 - 2 * c
    ahead = (lax.rem(z + 1, chips) * 2 + c, lax.rem(z + chips - 1, chips) * 2 + c)

    def wrapped(q):
        return lax.rem(q + 2 * chips, chips)

    def remote(src, dst, send, recv, to):
        return pltpu.make_async_remote_copy(
            src_ref=src, dst_ref=dst, send_sem=send, recv_sem=recv, device_id={"dp": to}, device_id_type=MESH
        )

    def sib_copy(layer, block):
        src = other.at[block, :, 1 - c] if layer else own_grads.at[block, :, 1 - c]
        return remote(src, sib[layer].at[block], sib_send.at[layer, block], sib_recv.at[layer, block], sibling)

    def loc_copy(block):
        return pltpu.make_async_copy(other.at[block, :, c], loc.at[block], loc_sem.at[block])

    def rs_copy(layer, s, way, k):
        slots = ring[layer][s]
        return remote(slots.at[way, k], slots.at[way, k + 1], rs_send.at[layer, s, way, k], rs_recv.at[layer, s, way, k], ahead[way])

    def terms(layer, block, q, way):
        lanes = slice(way * LANES, (way + 1) * LANES)
        mine = loc[block, q, :, lanes] if layer else own_grads[block, q, c, :, lanes]
        return mine.astype(F32) + sib[layer][block, q, :, lanes].astype(F32)

    def rs_chunk(way, k):
        return wrapped(z - 1 - k if way == 0 else z + 1 + k)

    def rs_first(layer, s):
        first, count = STREAMS[s]
        for block in range(first, first + count):
            sib_copy(layer, block).wait_recv()
            if layer:
                loc_copy(block).wait()
        for way in range(2):
            for i in range(count):
                ring[layer][s][way, 0, i] = terms(layer, first + i, rs_chunk(way, 0), way).astype(BF16)
            rs_copy(layer, s, way, 0).start()

    def rs_step(layer, s, k):
        first, count = STREAMS[s]
        for way in range(2):
            rs_copy(layer, s, way, k - 1).wait_recv()
            for i in range(count):
                so_far = ring[layer][s][way, k, i].astype(F32)
                ring[layer][s][way, k, i] = (so_far + terms(layer, first + i, rs_chunk(way, k), way)).astype(BF16)
            rs_copy(layer, s, way, k).start()

    def rs_last(layer, s):
        first, count = STREAMS[s]
        total = jnp.zeros((1, LANES), F32)
        for way in range(2):
            rs_copy(layer, s, way, chips - 2).wait_recv()
            for i in range(count):
                so_far = ring[layer][s][way, chips - 1, i].astype(F32)
                summed = (so_far + terms(layer, first + i, z, way)).astype(BF16)
                final[layer][first + i, :, way * LANES : (way + 1) * LANES] = summed
                total += jnp.sum(summed.astype(F32) ** 2, 0, keepdims=True)
        return total

    def place(layer, s, q, core, way):
        first, count = STREAMS[s]
        return out.at[pl.ds(layer * blocks + first, count), q, core, :, pl.ds(way * LANES, LANES)]

    def ag_copy(layer, s, way, k, src=None):
        q = wrapped(z - k if way == 0 else z + k)
        here = place(layer, s, q, c, way)
        return remote(here if src is None else src, here, ag_send.at[layer, s, way, k], ag_recv.at[layer, s, way, k], ahead[way])

    def ag_first_copy(layer, s, way):
        first, count = STREAMS[s]
        return ag_copy(layer, s, way, 0, final[layer].at[pl.ds(first, count), :, pl.ds(way * LANES, LANES)])

    def pass_copy(layer, s, way, k):
        here = place(layer, s, wrapped(z - k if way == 0 else z + k), c, way)
        return remote(here, here, pass_send.at[layer, s, way, k - 1], pass_recv.at[layer, s, way, k - 1], sibling)

    def fin_copies(layer):
        here = out.at[pl.ds(layer * blocks, blocks), z, c]
        return (
            pltpu.make_async_copy(final[layer], here, fin_sem.at[layer]),
            remote(final[layer], here, fin_send.at[layer], fin_recv.at[layer], sibling),
        )

    def ag_first(layer):
        for s in range(2):
            for way in range(2):
                ag_first_copy(layer, s, way).start()
        for copy in fin_copies(layer):
            copy.start()

    def ag_step(layer, s, k, go_on):
        for way in range(2):
            ag_copy(layer, s, way, k - 1).wait_recv()
            if go_on:
                ag_copy(layer, s, way, k).start()
            pass_copy(layer, s, way, k).start()

    def norm_copy(k):
        return remote(norm.at[me], norm.at[me], norm_send.at[k], norm_recv.at[k], lax.rem(me + k, group))

    @pl.when(j == 0)
    def _():
        barrier = pltpu.get_barrier_semaphore()

        def greet(k, _):
            pl.semaphore_signal(barrier, inc=1, device_id={"dp": lax.rem(me + k, group)}, device_id_type=MESH)
            return 0

        lax.fori_loop(1, group, greet, 0)
        pl.semaphore_wait(barrier, group - 1)
        for block in range(blocks):
            sib_copy(1, block).start()
            loc_copy(block).start()

        def start(rows):
            fresh = normed(h[rows, :])
            a[rows, :] = fresh
            a_t[:, rows] = fresh.T
            dy_t[:, rows] = dy[rows, :].T

        row_loop(tokens, start)
        rs_first(1, 0)

    @pl.when(j > 0)
    def _():
        rs_step(1, 0, j)

    down_t[...] = down[0].T

    def rows_of(rows):
        g = dot(a[rows, :], gate[0])
        u = dot(a[rows, :], up[0])
        dhid = dot(dy[rows, :], down_t[...]).astype(BF16).astype(F32)
        s = sigmoid(g)
        act = g * s
        hidden[rows, :] = (act * u).astype(BF16)
        both[rows, 0:BLOCK] = (dhid * u * (s + act * (1.0 - s))).astype(BF16)
        both[rows, BLOCK:] = (dhid * act).astype(BF16)

    row_loop(tokens, rows_of)

    @pl.when(j == 0)
    def _():
        rs_first(1, 1)

    @pl.when(j > 0)
    def _():
        rs_step(1, 1, j)

    put(own_grads, j, 0, dot(a_t[...], both[:, 0:BLOCK]).astype(BF16))
    put(own_grads, j, d, dot(a_t[...], both[:, BLOCK:]).astype(BF16))
    by_down = dot(dy_t[...], hidden[...])
    for t in range(d // BLOCK):
        put(own_grads, j, 2 * d + t * BLOCK, by_down[t * BLOCK : (t + 1) * BLOCK, :].T.astype(BF16))
    sib_copy(0, j).start()

    @pl.when(j == blocks - 1)
    def _():
        rs_first(0, 0)
        squares = rs_last(1, 0)
        rs_first(0, 1)
        squares += rs_last(1, 1)
        ag_first(1)

        def both_rings(k, _):
            for s in range(2):
                rs_step(0, s, k)
                ag_step(1, s, k, True)
            return 0

        lax.fori_loop(1, chips - 1, both_rings, 0)
        squares += rs_last(0, 0)
        squares += rs_last(0, 1)
        ag_first(0)
        norm[me] = jnp.broadcast_to(jnp.sum(squares, -1, keepdims=True), norm.shape[1:])

        def send_norm(k, _):
            norm_copy(k).start()
            return 0

        lax.fori_loop(1, group, send_norm, 0)
        for s in range(2):
            ag_step(1, s, chips - 1, False)

        def last_ring(k, _):
            for s in range(2):
                ag_step(0, s, k, True)
            return 0

        lax.fori_loop(1, chips - 1, last_ring, 0)
        for s in range(2):
            ag_step(0, s, chips - 1, False)

        def wait_norm(k, _):
            copy = norm_copy(k)
            copy.wait_send()
            remote(norm.at[lax.rem(me + group - k, group)], norm.at[lax.rem(me + group - k, group)], norm_send.at[k], norm_recv.at[k], sibling).wait_recv()
            return 0

        lax.fori_loop(1, group, wait_norm, 0)
        norm_out[...] = jnp.sum(norm[...], 0)

        for layer in range(2):

            def wait_sib(block, _, layer=layer):
                sib_copy(layer, block).wait_send()
                return 0

            lax.fori_loop(0, blocks, wait_sib, 0)
            keep, passed = fin_copies(layer)
            keep.wait()
            passed.wait_send()
            other_final = out.at[pl.ds(layer * blocks, blocks), z, 1 - c]
            remote(final[layer], other_final, fin_send.at[layer], fin_recv.at[layer], sibling).wait_recv()

            def wait_rings(k, _, layer=layer):
                for s in range(2):
                    for way in range(2):
                        rs_copy(layer, s, way, k).wait_send()
                        ag_copy(layer, s, way, k).wait_send()
                        passed = pass_copy(layer, s, way, k + 1)
                        passed.wait_send()
                        there = place(layer, s, wrapped(z - k - 1 if way == 0 else z + k + 1), 1 - c, way)
                        remote(there, there, pass_send.at[layer, s, way, k], pass_recv.at[layer, s, way, k], sibling).wait_recv()
                return 0

            lax.fori_loop(0, chips - 1, wait_rings, 0)


def exchange(group, h, dy, w_gate, w_up, w_down, other):
    tokens, d = h.shape
    blocks, chips = w_gate.shape[2] // BLOCK, group // 2
    height = 3 * d // group
    whole = pl.BlockSpec((tokens, d), lambda j: (0, 0), pipeline_mode=pl.Buffered(1))
    half = (blocks, chips, height, BLOCK)
    steps = chips - 1
    rings = [pltpu.VMEM((2, chips, count, height, LANES), BF16) for _, count in STREAMS]
    dma = pltpu.SemaphoreType.DMA
    return pl.pallas_call(
        functools.partial(exchange_kernel, group),
        out_shape=[
            jax.ShapeDtypeStruct((2 * blocks, chips, 2, height, BLOCK), BF16),
            jax.ShapeDtypeStruct((8, LANES), F32),
        ],
        grid=(blocks,),
        in_specs=[whole, whole] + block_specs(0, d) + [pl.BlockSpec(memory_space=pl.ANY)],
        out_specs=[pl.BlockSpec(memory_space=pl.ANY), pl.BlockSpec((8, LANES), lambda j: (0, 0))],
        scratch_shapes=[
            pltpu.VMEM((tokens, d), BF16),
            pltpu.VMEM((d, tokens), BF16),
            pltpu.VMEM((d, tokens), BF16),
            pltpu.VMEM((tokens, 2 * BLOCK), BF16),
            pltpu.VMEM((tokens, BLOCK), BF16),
            pltpu.VMEM((d, BLOCK), BF16),
            pltpu.VMEM((blocks, chips, 2, height, BLOCK), BF16),
            pltpu.VMEM(half, BF16),
            pltpu.VMEM(half, BF16),
            pltpu.VMEM(half, BF16),
            *rings,
            *rings,
            pltpu.VMEM((blocks, height, BLOCK), BF16),
            pltpu.VMEM((blocks, height, BLOCK), BF16),
            pltpu.VMEM((group, 8, LANES), F32),
            dma((2, blocks)),
            dma((2, blocks)),
            dma((blocks,)),
            dma((2, 2, 2, steps)),
            dma((2, 2, 2, steps)),
            dma((2, 2, 2, steps)),
            dma((2, 2, 2, steps)),
            dma((2, 2, 2, steps)),
            dma((2, 2, 2, steps)),
            dma((2,)),
            dma((2,)),
            dma((2,)),
            dma((group,)),
            dma((group,)),
        ],
        compiler_params=pltpu.CompilerParams(vmem_limit_bytes=VMEM, collective_id=0, has_side_effects=True),
        name="exchange",
    )(h, dy, w_gate, w_up, w_down, other)


def adamw_kernel(parts, d, factor, g, *refs):
    ws, ms, vs, new_ws, new_ms, new_vs = (refs[i : i + 3] for i in range(0, 18, 3))
    f = factor[0]

    def update(i, at, grad):
        grad = grad.astype(F32) * f
        m = 0.9 * ms[i][at] + 0.1 * grad
        v = 0.95 * vs[i][at] + 0.05 * grad * grad
        w = ws[i][at].astype(F32)
        new_ws[i][at] = (w - 0.02 * (m * lax.rsqrt(v + 1e-8) + 0.1 * w)).astype(BF16)
        new_ms[i][at] = m
        new_vs[i][at] = v

    def grad_rows(start):
        return g[0, start : start + BLOCK, :]

    for i in range(2):
        for t in range(d // BLOCK):
            update(i, (0, slice(t * BLOCK, (t + 1) * BLOCK), slice(None)), grad_rows(i * d + t * BLOCK))
    for t in range(d // BLOCK):
        update(2, (0, slice(None), slice(t * BLOCK, (t + 1) * BLOCK)), grad_rows(2 * d + t * BLOCK))


def adamw(factor, g, weights, m, v):
    layers, d, ff = weights[0].shape
    blocks = ff // BLOCK
    tall = pl.BlockSpec((1, d, BLOCK), lambda l, j: (l, 0, j))
    flat = pl.BlockSpec((1, BLOCK, d), lambda l, j: (l, j, 0))
    three = [tall, tall, flat]
    return pl.pallas_call(
        functools.partial(adamw_kernel, 1, d),
        out_shape=[jax.ShapeDtypeStruct(o.shape, o.dtype) for o in (*weights, *m, *v)],
        grid=(layers, blocks),
        in_specs=[pl.BlockSpec(memory_space=pltpu.SMEM), pl.BlockSpec((1, 3 * d, BLOCK), lambda l, j: (l * blocks + j, 0, 0))] + three * 3,
        out_specs=three * 3,
        compiler_params=pltpu.CompilerParams(vmem_limit_bytes=VMEM),
        name="adamw",
    )(factor, g, *weights, *m, *v)


def solution(mesh):
    group = mesh.shape["dp"]

    def step(x, dy, *arrays):
        weights, m, v = (arrays[i : i + 3] for i in (0, 3, 6))
        h = forward(x[0], *weights)
        g1, dh = backward(1, False, h, dy[0], *weights)
        blocks, rows, lanes = g1.shape
        g, squares = exchange(group, x[0], dh, *weights, g1.reshape(blocks, group // 2, 2, rows // group, lanes))
        g = g.reshape(2 * blocks, rows, lanes)
        factor = jnp.minimum(1.0, 0.5 * lax.rsqrt(squares[0, :1] / g.size + 1e-30))
        return tuple(adamw(factor, g, weights, m, v))

    return jax.shard_map(
        step,
        mesh=mesh,
        in_specs=(P(("rep", "dp"), None, None),) * 2 + (P(None, None, None),) * 9,
        out_specs=(P("rep", None, None),) * 9,
        check_vma=False,
    )
```

```python
import functools

import jax
import jax.numpy as jnp
from jax import lax
from jax.experimental import pallas as pl
from jax.experimental.pallas import tpu as pltpu
from jax.sharding import PartitionSpec as P

BLOCK = 256
ROWS = 512
VMEM = 64 * 1024 * 1024 - 65536
F32, BF16 = jnp.float32, jnp.bfloat16


def dot(a, b):
    return jnp.dot(a, b, preferred_element_type=F32)


def sigmoid(x):
    return 0.5 * jnp.tanh(0.5 * x) + 0.5


def inverse_rms(wide):
    return lax.rsqrt(jnp.mean(wide * wide, -1, keepdims=True) + 1e-6)


def normed(h):
    wide = h.astype(F32)
    return (wide * inverse_rms(wide)).astype(BF16)


def row_loop(tokens, body):
    for i in range(tokens // ROWS):
        body(slice(i * ROWS, (i + 1) * ROWS))


def forward_kernel(x, gate, up, down, out, a, total):
    tokens = x.shape[0]
    j = pl.program_id(0)

    @pl.when(j == 0)
    def _():
        def start(rows):
            a[rows, :] = normed(x[rows, :])
            total[rows, :] = jnp.zeros((ROWS, total.shape[1]), F32)

        row_loop(tokens, start)

    def rows_of(rows):
        g = dot(a[rows, :], gate[0])
        u = dot(a[rows, :], up[0])
        hidden = (g * sigmoid(g) * u).astype(BF16)
        total[rows, :] += dot(hidden, down[0])

    row_loop(tokens, rows_of)

    @pl.when(j == pl.num_programs(0) - 1)
    def _():
        def finish(rows):
            out[rows, :] = x[rows, :] + total[rows, :].astype(BF16)

        row_loop(tokens, finish)


def block_specs(layer, d):
    return [
        pl.BlockSpec((1, d, BLOCK), lambda j: (layer, 0, j)),
        pl.BlockSpec((1, d, BLOCK), lambda j: (layer, 0, j)),
        pl.BlockSpec((1, BLOCK, d), lambda j: (layer, j, 0)),
    ]


def forward(x, w_gate, w_up, w_down):
    tokens, d = x.shape
    blocks = w_gate.shape[2] // BLOCK
    whole = pl.BlockSpec((tokens, d), lambda j: (0, 0))
    return pl.pallas_call(
        forward_kernel,
        out_shape=jax.ShapeDtypeStruct((tokens, d), BF16),
        grid=(blocks,),
        in_specs=[whole] + block_specs(0, d),
        out_specs=whole,
        scratch_shapes=[pltpu.VMEM((tokens, d), BF16), pltpu.VMEM((tokens, d), F32)],
        compiler_params=pltpu.CompilerParams(vmem_limit_bytes=VMEM),
        name="forward",
    )(x, w_gate, w_up, w_down)


MESH = pl.DeviceIdType.MESH
LANES = 128
STREAMS = ((0, 2, 5), (2, 2, 9), (4, 3, 15), (7, 3, 21), (10, 2, 25), (12, 2, 28))


def backward_kernel(group, blocks, h1, x, dy, gate, up, down, out, norm_out, *scratch):
    (h, by, a, a_t, by_t, both, hidden, down_t, w_t, total, terms, sib, norm, squares), scratch = scratch[:14], scratch[14:]
    ring, scratch = scratch[: len(STREAMS)], scratch[len(STREAMS) :]
    final, sems = scratch[: len(STREAMS)], scratch[len(STREAMS) :]
    load_sem, sib_send, sib_recv, rs_send, rs_recv, ag_send, ag_recv, pass_send, pass_recv, fin_sem, fin_send, fin_recv, norm_send, norm_recv = sems
    tokens, d = h.shape
    height = terms.shape[2]
    all_blocks = 2 * blocks
    chips = group // 2
    t = pl.program_id(0)
    p = lax.div(t, 2)
    me = lax.axis_index("dp")
    z, c = lax.div(me, 2), lax.rem(me, 2)
    sibling = me + 1 - 2 * c
    ahead = (lax.rem(z + 1, chips) * 2 + c, lax.rem(z + chips - 1, chips) * 2 + c)

    def wrapped(q):
        return lax.rem(q + 2 * chips, chips)

    def remote(src, dst, send, recv, to):
        return pltpu.make_async_remote_copy(
            src_ref=src, dst_ref=dst, send_sem=send, recv_sem=recv, device_id={"dp": to}, device_id_type=MESH
        )

    def outbox(block):
        return all_blocks + lax.rem(block, 2)

    def put(row, value):
        done = 0
        while done < value.shape[0]:
            piece, at = divmod(row + done, height)
            size = min(height - at, value.shape[0] - done)
            mine = c if piece % 2 else 1 - c
            index = mine * p + (1 - mine) * outbox(p)
            terms[index, piece // 2, at : at + size, :] = value[done : done + size, :]
            done += size

    def sib_copy(block):
        return remote(terms.at[outbox(block)], sib.at[block], sib_send.at[block], sib_recv.at[block], sibling)

    def rs_copy(s, way, k):
        return remote(ring[s].at[way, k], ring[s].at[way, k + 1], rs_send.at[s, way, k], rs_recv.at[s, way, k], ahead[way])

    def own_terms(block, q, way):
        lanes = slice(way * LANES, (way + 1) * LANES)
        return terms[block, q, :, lanes].astype(F32) + sib[block, q, :, lanes].astype(F32)

    def rs_chunk(way, k):
        return wrapped(z - 1 - k if way == 0 else z + 1 + k)

    def rs_first(s):
        first, count, _ = STREAMS[s]
        for block in range(first, first + count):
            sib_copy(block).wait_recv()
        for way in range(2):
            for i in range(count):
                ring[s][way, 0, i] = own_terms(first + i, rs_chunk(way, 0), way).astype(BF16)
            rs_copy(s, way, 0).start()

    def rs_step(s, k):
        first, count, _ = STREAMS[s]
        for way in range(2):
            rs_copy(s, way, k - 1).wait_recv()
            for i in range(count):
                so_far = ring[s][way, k, i].astype(F32)
                ring[s][way, k, i] = (so_far + own_terms(first + i, rs_chunk(way, k), way)).astype(BF16)
            rs_copy(s, way, k).start()

    def rs_last(s):
        first, count, _ = STREAMS[s]
        for way in range(2):
            rs_copy(s, way, chips - 2).wait_recv()
            for i in range(count):
                so_far = ring[s][way, chips - 1, i].astype(F32)
                summed = (so_far + own_terms(first + i, z, way)).astype(BF16)
                final[s][i, :, way * LANES : (way + 1) * LANES] = summed
                wide = summed.astype(F32)
                squares[...] += jnp.sum(wide * wide, 0, keepdims=True)

    def place(s, q, core, way):
        first, count, _ = STREAMS[s]
        return out.at[pl.ds(first, count), q, core, :, pl.ds(way * LANES, LANES)]

    def ag_chunk(way, k):
        return wrapped(z - k if way == 0 else z + k)

    def ag_copy(s, way, k, src=None):
        here = place(s, ag_chunk(way, k), c, way)
        return remote(here if src is None else src, here, ag_send.at[s, way, k], ag_recv.at[s, way, k], ahead[way])

    def pass_copy(s, way, k):
        here = place(s, ag_chunk(way, k), c, way)
        return remote(here, here, pass_send.at[s, way, k - 1], pass_recv.at[s, way, k - 1], sibling)

    def fin_place(s, core):
        first, count, _ = STREAMS[s]
        return out.at[pl.ds(first, count), z, core]

    def fin_copies(s):
        return (
            pltpu.make_async_copy(final[s], fin_place(s, c), fin_sem.at[s]),
            remote(final[s], fin_place(s, c), fin_send.at[s], fin_recv.at[s], sibling),
        )

    def ag_first(s):
        for way in range(2):
            ag_copy(s, way, 0, final[s].at[:, :, pl.ds(way * LANES, LANES)]).start()
        for copy in fin_copies(s):
            copy.start()

    def ag_step(s, k, go_on):
        for way in range(2):
            ag_copy(s, way, k - 1).wait_recv()
            if go_on:
                ag_copy(s, way, k).start()
            pass_copy(s, way, k).start()

    def norm_copy(k):
        return remote(norm.at[me], norm.at[me], norm_send.at[k], norm_recv.at[k], lax.rem(me + k, group))

    def norm_arrival(k):
        place = norm.at[lax.rem(me + group - k, group)]
        return remote(place, place, norm_send.at[k], norm_recv.at[k], sibling)

    def loads(layer_input, by_output=None):
        copies = [pltpu.make_async_copy(layer_input, h, load_sem.at[0])]
        if by_output is not None:
            copies.append(pltpu.make_async_copy(by_output, by, load_sem.at[1]))
        return copies

    def prepare(rows):
        fresh = normed(h[rows, :])
        a[rows, :] = fresh
        a_t[:, rows] = fresh.T
        by_t[:, rows] = by[rows, :].T

    @pl.when(t == 0)
    def _():
        for copy in loads(h1, dy):
            copy.start()
        barrier = pltpu.get_barrier_semaphore()

        def greet(k, _):
            pl.semaphore_signal(barrier, inc=1, device_id={"dp": lax.rem(me + k, group)}, device_id_type=MESH)
            return 0

        lax.fori_loop(1, group, greet, 0)
        squares[...] = jnp.zeros(squares.shape, F32)
        for copy in loads(h1, dy):
            copy.wait()

        def start(rows):
            prepare(rows)
            total[rows, :] = jnp.zeros((ROWS, d), F32)

        row_loop(tokens, start)
        pl.semaphore_wait(barrier, group - 1)

    for s, (_, _, first_slot) in enumerate(STREAMS):
        k = t - first_slot

        @pl.when(k == 0)
        def _(s=s):
            rs_first(s)

        @pl.when((k > 0) & (k < chips - 1))
        def _(s=s, k=k):
            rs_step(s, k)

        @pl.when(k == chips - 1)
        def _(s=s):
            rs_last(s)
            ag_first(s)
            if s == len(STREAMS) - 1:
                norm[me] = jnp.broadcast_to(jnp.sum(squares[...], -1, keepdims=True), norm.shape[1:])

                def send(i, _):
                    norm_copy(i).start()
                    return 0

                lax.fori_loop(1, group, send, 0)

        @pl.when((k > chips - 1) & (k < 2 * chips - 2))
        def _(s=s, k=k):
            ag_step(s, k - (chips - 1), True)

        @pl.when(k == 2 * chips - 2)
        def _(s=s):
            ag_step(s, chips - 1, False)

    @pl.when(t == all_blocks)
    def _():
        def by_input(rows):
            wide = h[rows, :].astype(F32)
            scale = inverse_rms(wide)
            by_a = total[rows, :].astype(BF16).astype(F32)
            by_scale = jnp.sum(by_a * wide, -1, keepdims=True)
            by_h = by_a * scale - wide * (scale * scale * scale * by_scale / d)
            by[rows, :] += by_h.astype(BF16)

        row_loop(tokens, by_input)
        for copy in loads(x):
            copy.start()
            copy.wait()
        row_loop(tokens, prepare)

    @pl.when((t < 2 * all_blocks) & (lax.rem(t, 2) == 0))
    def _():
        down_t[...] = down[0].T

        def rows_of(rows):
            g = dot(a[rows, :], gate[0])
            u = dot(a[rows, :], up[0])
            by_hidden = dot(by[rows, :], down_t[...]).astype(BF16).astype(F32)
            s = sigmoid(g)
            act = g * s
            hidden[rows, :] = (act * u).astype(BF16)
            both[rows, 0:BLOCK] = (by_hidden * u * (s + act * (1.0 - s))).astype(BF16)
            both[rows, BLOCK:] = (by_hidden * act).astype(BF16)

        row_loop(tokens, rows_of)

    @pl.when((t < 2 * all_blocks) & (lax.rem(t, 2) == 1))
    def _():
        @pl.when(p >= 2)
        def _():
            sib_copy(p - 2).wait_send()

        put(0, dot(a_t[...], both[:, 0:BLOCK]).astype(BF16))
        put(d, dot(a_t[...], both[:, BLOCK:]).astype(BF16))
        by_down = dot(by_t[...], hidden[...])
        for i in range(d // BLOCK):
            put(2 * d + i * BLOCK, by_down[i * BLOCK : (i + 1) * BLOCK, :].T.astype(BF16))
        sib_copy(p).start()

        @pl.when(p < blocks)
        def _():
            w_t[0:BLOCK, :] = gate[0].T
            w_t[BLOCK:, :] = up[0].T

            def by_normed(rows):
                total[rows, :] += dot(both[rows, :], w_t[...])

            row_loop(tokens, by_normed)

    @pl.when(t == pl.num_programs(0) - 1)
    def _():
        def wait_norm(k, _):
            norm_copy(k).wait_send()
            norm_arrival(k).wait_recv()
            return 0

        lax.fori_loop(1, group, wait_norm, 0)
        norm_out[...] = jnp.sum(norm[...], 0)
        for block in range(all_blocks - 2, all_blocks):
            sib_copy(block).wait_send()
        for s in range(len(STREAMS)):
            keep, passed = fin_copies(s)
            keep.wait()
            passed.wait_send()
            remote(final[s], fin_place(s, 1 - c), fin_send.at[s], fin_recv.at[s], sibling).wait_recv()

            def wait_rings(k, _, s=s):
                for way in range(2):
                    rs_copy(s, way, k).wait_send()
                    ag_copy(s, way, k).wait_send()
                    pass_copy(s, way, k + 1).wait_send()
                    there = place(s, ag_chunk(way, k + 1), 1 - c, way)
                    remote(there, there, pass_send.at[s, way, k], pass_recv.at[s, way, k], sibling).wait_recv()
                return 0

            lax.fori_loop(0, chips - 1, wait_rings, 0)


def backward(group, h1, x, dy, w_gate, w_up, w_down):
    tokens, d = x.shape
    layers = w_gate.shape[0]
    blocks, chips = w_gate.shape[2] // BLOCK, group // 2
    height = 3 * d // group
    steps = chips - 1

    def layer_block(t):
        p = jnp.minimum(lax.div(t, 2), layers * blocks - 1)
        return layers - 1 - lax.div(p, blocks), lax.rem(p, blocks)

    def tall(t):
        layer, j = layer_block(t)
        return layer, 0, j

    def flat(t):
        layer, j = layer_block(t)
        return layer, j, 0

    anywhere = pl.BlockSpec(memory_space=pl.ANY)
    dma = pltpu.SemaphoreType.DMA
    rows = pltpu.VMEM((tokens, d), BF16)
    columns = pltpu.VMEM((d, tokens), BF16)
    ring_sems = [dma((len(STREAMS), 2, steps))] * 6
    return pl.pallas_call(
        functools.partial(backward_kernel, group, blocks),
        out_shape=[
            jax.ShapeDtypeStruct((layers * blocks, chips, 2, height, BLOCK), BF16),
            jax.ShapeDtypeStruct((8, LANES), F32),
        ],
        grid=(STREAMS[-1][2] + 2 * steps + 1,),
        in_specs=[anywhere] * 3
        + [pl.BlockSpec((1, d, BLOCK), tall), pl.BlockSpec((1, d, BLOCK), tall), pl.BlockSpec((1, BLOCK, d), flat)],
        out_specs=[anywhere, pl.BlockSpec((8, LANES), lambda t: (0, 0))],
        scratch_shapes=[
            rows,
            rows,
            rows,
            columns,
            columns,
            pltpu.VMEM((tokens, 2 * BLOCK), BF16),
            pltpu.VMEM((tokens, BLOCK), BF16),
            pltpu.VMEM((d, BLOCK), BF16),
            pltpu.VMEM((2 * BLOCK, d), BF16),
            pltpu.VMEM((tokens, d), F32),
            pltpu.VMEM((layers * blocks + 2, chips, height, BLOCK), BF16),
            pltpu.VMEM((layers * blocks, chips, height, BLOCK), BF16),
            pltpu.VMEM((group, 8, LANES), F32),
            pltpu.VMEM((1, LANES), F32),
            *[pltpu.VMEM((2, chips, count, height, LANES), BF16) for _, count, _ in STREAMS],
            *[pltpu.VMEM((count, height, BLOCK), BF16) for _, count, _ in STREAMS],
            dma((2,)),
            dma((layers * blocks,)),
            dma((layers * blocks,)),
            *ring_sems,
            *[dma((len(STREAMS),))] * 3,
            dma((group,)),
            dma((group,)),
        ],
        compiler_params=pltpu.CompilerParams(vmem_limit_bytes=VMEM, collective_id=0, has_side_effects=True),
        name="backward",
    )(h1, x, dy, w_gate, w_up, w_down)


def adamw_kernel(parts, d, factor, g, *refs):
    ws, ms, vs, new_ws, new_ms, new_vs = (refs[i : i + 3] for i in range(0, 18, 3))
    f = factor[0]

    def update(i, at, grad):
        grad = grad.astype(F32) * f
        m = 0.9 * ms[i][at] + 0.1 * grad
        v = 0.95 * vs[i][at] + 0.05 * grad * grad
        w = ws[i][at].astype(F32)
        new_ws[i][at] = (w - 0.02 * (m * lax.rsqrt(v + 1e-8) + 0.1 * w)).astype(BF16)
        new_ms[i][at] = m
        new_vs[i][at] = v

    def grad_rows(start):
        return g[0, start : start + BLOCK, :]

    for i in range(2):
        for t in range(d // BLOCK):
            update(i, (0, slice(t * BLOCK, (t + 1) * BLOCK), slice(None)), grad_rows(i * d + t * BLOCK))
    for t in range(d // BLOCK):
        update(2, (0, slice(None), slice(t * BLOCK, (t + 1) * BLOCK)), grad_rows(2 * d + t * BLOCK))


def adamw(factor, g, weights, m, v):
    layers, d, ff = weights[0].shape
    blocks = ff // BLOCK
    tall = pl.BlockSpec((1, d, BLOCK), lambda l, j: (l, 0, j))
    flat = pl.BlockSpec((1, BLOCK, d), lambda l, j: (l, j, 0))
    three = [tall, tall, flat]
    return pl.pallas_call(
        functools.partial(adamw_kernel, 1, d),
        out_shape=[jax.ShapeDtypeStruct(o.shape, o.dtype) for o in (*weights, *m, *v)],
        grid=(layers, blocks),
        in_specs=[pl.BlockSpec(memory_space=pltpu.SMEM), pl.BlockSpec((1, 3 * d, BLOCK), lambda l, j: ((layers - 1 - l) * blocks + j, 0, 0))] + three * 3,
        out_specs=three * 3,
        compiler_params=pltpu.CompilerParams(vmem_limit_bytes=VMEM),
        name="adamw",
    )(factor, g, *weights, *m, *v)


def solution(mesh):
    group = mesh.shape["dp"]

    def step(x, dy, *arrays):
        weights, m, v = (arrays[i : i + 3] for i in (0, 3, 6))
        h1 = forward(x[0], *weights)
        g, squares = backward(group, h1, x[0], dy[0], *weights)
        g = g.reshape(g.shape[0], -1, g.shape[-1])
        factor = jnp.minimum(1.0, 0.5 * lax.rsqrt(squares[0, :1] / g.size + 1e-30))
        return tuple(adamw(factor, g, weights, m, v))

    return jax.shard_map(
        step,
        mesh=mesh,
        in_specs=(P(("rep", "dp"), None, None),) * 2 + (P(None, None, None),) * 9,
        out_specs=(P("rep", None, None),) * 9,
        check_vma=False,
    )
```

```python
import functools

import jax
import jax.numpy as jnp
from jax import lax
from jax.experimental import pallas as pl
from jax.experimental.pallas import tpu as pltpu
from jax.sharding import PartitionSpec as P

BLOCK = 256
ROWS = 512
VMEM = 64 * 1024 * 1024 - 65536
F32, BF16 = jnp.float32, jnp.bfloat16


def dot(a, b):
    return jnp.dot(a, b, preferred_element_type=F32)


def sigmoid(x):
    return 0.5 * jnp.tanh(0.5 * x) + 0.5


def inverse_rms(wide):
    return lax.rsqrt(jnp.mean(wide * wide, -1, keepdims=True) + 1e-6)


def normed(h):
    wide = h.astype(F32)
    return (wide * inverse_rms(wide)).astype(BF16)


def row_loop(tokens, body):
    for i in range(tokens // ROWS):
        body(slice(i * ROWS, (i + 1) * ROWS))


def forward_kernel(x, gate, up, down, out, a, total):
    tokens = x.shape[0]
    j = pl.program_id(0)

    @pl.when(j == 0)
    def _():
        def start(rows):
            a[rows, :] = normed(x[rows, :])
            total[rows, :] = jnp.zeros((ROWS, total.shape[1]), F32)

        row_loop(tokens, start)

    def rows_of(rows):
        g = dot(a[rows, :], gate[0])
        u = dot(a[rows, :], up[0])
        hidden = (g * sigmoid(g) * u).astype(BF16)
        total[rows, :] += dot(hidden, down[0])

    row_loop(tokens, rows_of)

    @pl.when(j == pl.num_programs(0) - 1)
    def _():
        def finish(rows):
            out[rows, :] = x[rows, :] + total[rows, :].astype(BF16)

        row_loop(tokens, finish)


def block_specs(layer, d):
    return [
        pl.BlockSpec((1, d, BLOCK), lambda j: (layer, 0, j)),
        pl.BlockSpec((1, d, BLOCK), lambda j: (layer, 0, j)),
        pl.BlockSpec((1, BLOCK, d), lambda j: (layer, j, 0)),
    ]


def forward(x, w_gate, w_up, w_down):
    tokens, d = x.shape
    blocks = w_gate.shape[2] // BLOCK
    whole = pl.BlockSpec((tokens, d), lambda j: (0, 0))
    return pl.pallas_call(
        forward_kernel,
        out_shape=jax.ShapeDtypeStruct((tokens, d), BF16),
        grid=(blocks,),
        in_specs=[whole] + block_specs(0, d),
        out_specs=whole,
        scratch_shapes=[pltpu.VMEM((tokens, d), BF16), pltpu.VMEM((tokens, d), F32)],
        compiler_params=pltpu.CompilerParams(vmem_limit_bytes=VMEM),
        name="forward",
    )(x, w_gate, w_up, w_down)


MESH = pl.DeviceIdType.MESH
LANES = 128
STREAMS = (
    (0, 2, 5, 16),
    (2, 2, 8, 15),
    (4, 2, 12, 23),
    (6, 1, 14, 21),
    (7, 2, 19, 35),
    (9, 2, 23, 35),
    (11, 2, 26, 35),
    (13, 1, 28, 35),
)


def backward_kernel(group, blocks, h1, x, dy, gate, up, down, out, norm_out, *scratch):
    (h, by, a, a_t, by_t, both, hidden, down_t, w_t, total, terms, sib, norm, squares), scratch = scratch[:14], scratch[14:]
    ring, scratch = scratch[: len(STREAMS)], scratch[len(STREAMS) :]
    final, sems = scratch[: len(STREAMS)], scratch[len(STREAMS) :]
    load_sem, sib_send, sib_recv, rs_send, rs_recv, ag_send, ag_recv, pass_send, pass_recv, fin_sem, fin_send, fin_recv, norm_send, norm_recv = sems
    tokens, d = h.shape
    height = terms.shape[2]
    all_blocks = 2 * blocks
    chips = group // 2
    t = pl.program_id(0)
    p = lax.div(t, 2)
    me = lax.axis_index("dp")
    z, c = lax.div(me, 2), lax.rem(me, 2)
    sibling = me + 1 - 2 * c
    ahead = (lax.rem(z + 1, chips) * 2 + c, lax.rem(z + chips - 1, chips) * 2 + c)

    def wrapped(q):
        return lax.rem(q + 2 * chips, chips)

    def remote(src, dst, send, recv, to):
        return pltpu.make_async_remote_copy(
            src_ref=src, dst_ref=dst, send_sem=send, recv_sem=recv, device_id={"dp": to}, device_id_type=MESH
        )

    def outbox(block):
        return all_blocks + lax.rem(block, 2)

    def put(row, value):
        done = 0
        while done < value.shape[0]:
            piece, at = divmod(row + done, height)
            size = min(height - at, value.shape[0] - done)
            mine = c if piece % 2 else 1 - c
            index = mine * p + (1 - mine) * outbox(p)
            terms[index, piece // 2, at : at + size, :] = value[done : done + size, :]
            done += size

    def sib_copy(block):
        return remote(terms.at[outbox(block)], sib.at[block], sib_send.at[block], sib_recv.at[block], sibling)

    def rs_copy(s, way, k):
        return remote(ring[s].at[way, k], ring[s].at[way, k + 1], rs_send.at[s, way, k], rs_recv.at[s, way, k], ahead[way])

    def own_terms(block, q, way):
        lanes = slice(way * LANES, (way + 1) * LANES)
        return terms[block, q, :, lanes].astype(F32) + sib[block, q, :, lanes].astype(F32)

    def rs_chunk(way, k):
        return wrapped(z - 1 - k if way == 0 else z + 1 + k)

    def rs_first(s):
        first, count = STREAMS[s][:2]
        for block in range(first, first + count):
            sib_copy(block).wait_recv()
        for way in range(2):
            for i in range(count):
                ring[s][way, 0, i] = own_terms(first + i, rs_chunk(way, 0), way).astype(BF16)
            rs_copy(s, way, 0).start()

    def rs_step(s, k):
        first, count = STREAMS[s][:2]
        for way in range(2):
            rs_copy(s, way, k - 1).wait_recv()
            for i in range(count):
                so_far = ring[s][way, k, i].astype(F32)
                ring[s][way, k, i] = (so_far + own_terms(first + i, rs_chunk(way, k), way)).astype(BF16)
            rs_copy(s, way, k).start()

    def rs_last(s):
        first, count = STREAMS[s][:2]
        for way in range(2):
            rs_copy(s, way, chips - 2).wait_recv()
            for i in range(count):
                so_far = ring[s][way, chips - 1, i].astype(F32)
                summed = (so_far + own_terms(first + i, z, way)).astype(BF16)
                final[s][i, :, way * LANES : (way + 1) * LANES] = summed
                wide = summed.astype(F32)
                squares[...] += jnp.sum(wide * wide, 0, keepdims=True)

    def place(s, q, core, way):
        first, count = STREAMS[s][:2]
        return out.at[pl.ds(first, count), q, core, :, pl.ds(way * LANES, LANES)]

    def ag_chunk(way, k):
        return wrapped(z - k if way == 0 else z + k)

    def ag_copy(s, way, k, src=None):
        here = place(s, ag_chunk(way, k), c, way)
        return remote(here if src is None else src, here, ag_send.at[s, way, k], ag_recv.at[s, way, k], ahead[way])

    def pass_copy(s, way, k):
        here = place(s, ag_chunk(way, k), c, way)
        return remote(here, here, pass_send.at[s, way, k - 1], pass_recv.at[s, way, k - 1], sibling)

    def fin_place(s, core):
        first, count = STREAMS[s][:2]
        return out.at[pl.ds(first, count), z, core]

    def fin_copies(s):
        return (
            pltpu.make_async_copy(final[s], fin_place(s, c), fin_sem.at[s]),
            remote(final[s], fin_place(s, c), fin_send.at[s], fin_recv.at[s], sibling),
        )

    def ag_first(s):
        for way in range(2):
            ag_copy(s, way, 0, final[s].at[:, :, pl.ds(way * LANES, LANES)]).start()
        for copy in fin_copies(s):
            copy.start()

    def ag_step(s, k, go_on):
        for way in range(2):
            ag_copy(s, way, k - 1).wait_recv()
            if go_on:
                ag_copy(s, way, k).start()
            pass_copy(s, way, k).start()

    def norm_copy(k):
        return remote(norm.at[me], norm.at[me], norm_send.at[k], norm_recv.at[k], lax.rem(me + k, group))

    def norm_arrival(k):
        place = norm.at[lax.rem(me + group - k, group)]
        return remote(place, place, norm_send.at[k], norm_recv.at[k], sibling)

    def loads(layer_input, by_output=None):
        copies = [pltpu.make_async_copy(layer_input, h, load_sem.at[0])]
        if by_output is not None:
            copies.append(pltpu.make_async_copy(by_output, by, load_sem.at[1]))
        return copies

    def prepare(rows):
        fresh = normed(h[rows, :])
        a[rows, :] = fresh
        a_t[:, rows] = fresh.T
        by_t[:, rows] = by[rows, :].T

    @pl.when(t == 0)
    def _():
        for copy in loads(h1, dy):
            copy.start()
        barrier = pltpu.get_barrier_semaphore()

        def greet(k, _):
            pl.semaphore_signal(barrier, inc=1, device_id={"dp": lax.rem(me + k, group)}, device_id_type=MESH)
            return 0

        lax.fori_loop(1, group, greet, 0)
        squares[...] = jnp.zeros(squares.shape, F32)
        for copy in loads(h1, dy):
            copy.wait()

        def start(rows):
            prepare(rows)
            total[rows, :] = jnp.zeros((ROWS, d), F32)

        row_loop(tokens, start)
        pl.semaphore_wait(barrier, group - 1)

    for s, (_, _, sums_slot, results_slot) in enumerate(STREAMS):
        k = t - sums_slot

        @pl.when(k == 0)
        def _(s=s):
            rs_first(s)

        @pl.when((k > 0) & (k < chips - 1))
        def _(s=s, k=k):
            rs_step(s, k)

        @pl.when(k == chips - 1)
        def _(s=s):
            rs_last(s)
            if s == len(STREAMS) - 1:
                norm[me] = jnp.broadcast_to(jnp.sum(squares[...], -1, keepdims=True), norm.shape[1:])

                def send(i, _):
                    norm_copy(i).start()
                    return 0

                lax.fori_loop(1, group, send, 0)

        k = t - results_slot

        @pl.when(k == 0)
        def _(s=s):
            ag_first(s)

        @pl.when((k > 0) & (k < chips - 1))
        def _(s=s, k=k):
            ag_step(s, k, True)

        @pl.when(k == chips - 1)
        def _(s=s):
            ag_step(s, chips - 1, False)

    @pl.when(t == all_blocks)
    def _():
        def by_input(rows):
            wide = h[rows, :].astype(F32)
            scale = inverse_rms(wide)
            by_a = total[rows, :].astype(BF16).astype(F32)
            by_scale = jnp.sum(by_a * wide, -1, keepdims=True)
            by_h = by_a * scale - wide * (scale * scale * scale * by_scale / d)
            by[rows, :] += by_h.astype(BF16)

        row_loop(tokens, by_input)
        for copy in loads(x):
            copy.start()
            copy.wait()
        row_loop(tokens, prepare)

    @pl.when((t < 2 * all_blocks) & (lax.rem(t, 2) == 0))
    def _():
        down_t[...] = down[0].T

        def rows_of(rows):
            g = dot(a[rows, :], gate[0])
            u = dot(a[rows, :], up[0])
            by_hidden = dot(by[rows, :], down_t[...]).astype(BF16).astype(F32)
            s = sigmoid(g)
            act = g * s
            hidden[rows, :] = (act * u).astype(BF16)
            both[rows, 0:BLOCK] = (by_hidden * u * (s + act * (1.0 - s))).astype(BF16)
            both[rows, BLOCK:] = (by_hidden * act).astype(BF16)

        row_loop(tokens, rows_of)

    @pl.when((t < 2 * all_blocks) & (lax.rem(t, 2) == 1))
    def _():
        @pl.when(p >= 2)
        def _():
            sib_copy(p - 2).wait_send()

        put(0, dot(a_t[...], both[:, 0:BLOCK]).astype(BF16))
        put(d, dot(a_t[...], both[:, BLOCK:]).astype(BF16))
        by_down = dot(by_t[...], hidden[...])
        for i in range(d // BLOCK):
            put(2 * d + i * BLOCK, by_down[i * BLOCK : (i + 1) * BLOCK, :].T.astype(BF16))
        sib_copy(p).start()

        @pl.when(p < blocks)
        def _():
            w_t[0:BLOCK, :] = gate[0].T
            w_t[BLOCK:, :] = up[0].T

            def by_normed(rows):
                total[rows, :] += dot(both[rows, :], w_t[...])

            row_loop(tokens, by_normed)

    @pl.when(t == pl.num_programs(0) - 1)
    def _():
        def wait_norm(k, _):
            norm_copy(k).wait_send()
            norm_arrival(k).wait_recv()
            return 0

        lax.fori_loop(1, group, wait_norm, 0)
        norm_out[...] = jnp.sum(norm[...], 0)
        for block in range(all_blocks - 2, all_blocks):
            sib_copy(block).wait_send()
        for s in range(len(STREAMS)):
            keep, passed = fin_copies(s)
            keep.wait()
            passed.wait_send()
            remote(final[s], fin_place(s, 1 - c), fin_send.at[s], fin_recv.at[s], sibling).wait_recv()

            def wait_rings(k, _, s=s):
                for way in range(2):
                    rs_copy(s, way, k).wait_send()
                    ag_copy(s, way, k).wait_send()
                    pass_copy(s, way, k + 1).wait_send()
                    there = place(s, ag_chunk(way, k + 1), 1 - c, way)
                    remote(there, there, pass_send.at[s, way, k], pass_recv.at[s, way, k], sibling).wait_recv()
                return 0

            lax.fori_loop(0, chips - 1, wait_rings, 0)


def backward(group, h1, x, dy, w_gate, w_up, w_down):
    tokens, d = x.shape
    layers = w_gate.shape[0]
    blocks, chips = w_gate.shape[2] // BLOCK, group // 2
    height = 3 * d // group
    steps = chips - 1

    def layer_block(t):
        p = jnp.minimum(lax.div(t, 2), layers * blocks - 1)
        return layers - 1 - lax.div(p, blocks), lax.rem(p, blocks)

    def tall(t):
        layer, j = layer_block(t)
        return layer, 0, j

    def flat(t):
        layer, j = layer_block(t)
        return layer, j, 0

    anywhere = pl.BlockSpec(memory_space=pl.ANY)
    dma = pltpu.SemaphoreType.DMA
    rows = pltpu.VMEM((tokens, d), BF16)
    columns = pltpu.VMEM((d, tokens), BF16)
    ring_sems = [dma((len(STREAMS), 2, steps))] * 6
    return pl.pallas_call(
        functools.partial(backward_kernel, group, blocks),
        out_shape=[
            jax.ShapeDtypeStruct((layers * blocks, chips, 2, height, BLOCK), BF16),
            jax.ShapeDtypeStruct((8, LANES), F32),
        ],
        grid=(max(slot for *_, slot in STREAMS) + chips,),
        in_specs=[anywhere] * 3
        + [pl.BlockSpec((1, d, BLOCK), tall), pl.BlockSpec((1, d, BLOCK), tall), pl.BlockSpec((1, BLOCK, d), flat)],
        out_specs=[anywhere, pl.BlockSpec((8, LANES), lambda t: (0, 0))],
        scratch_shapes=[
            rows,
            rows,
            rows,
            columns,
            columns,
            pltpu.VMEM((tokens, 2 * BLOCK), BF16),
            pltpu.VMEM((tokens, BLOCK), BF16),
            pltpu.VMEM((d, BLOCK), BF16),
            pltpu.VMEM((2 * BLOCK, d), BF16),
            pltpu.VMEM((tokens, d), F32),
            pltpu.VMEM((layers * blocks + 2, chips, height, BLOCK), BF16),
            pltpu.VMEM((layers * blocks, chips, height, BLOCK), BF16),
            pltpu.VMEM((group, 8, LANES), F32),
            pltpu.VMEM((1, LANES), F32),
            *[pltpu.VMEM((2, chips, count, height, LANES), BF16) for _, count, *_ in STREAMS],
            *[pltpu.VMEM((count, height, BLOCK), BF16) for _, count, *_ in STREAMS],
            dma((2,)),
            dma((layers * blocks,)),
            dma((layers * blocks,)),
            *ring_sems,
            *[dma((len(STREAMS),))] * 3,
            dma((group,)),
            dma((group,)),
        ],
        compiler_params=pltpu.CompilerParams(vmem_limit_bytes=VMEM, collective_id=0, has_side_effects=True),
        name="backward",
    )(h1, x, dy, w_gate, w_up, w_down)


def adamw_kernel(parts, d, factor, g, *refs):
    ws, ms, vs, new_ws, new_ms, new_vs = (refs[i : i + 3] for i in range(0, 18, 3))
    f = factor[0]

    def update(i, at, grad):
        grad = grad.astype(F32) * f
        m = 0.9 * ms[i][at] + 0.1 * grad
        v = 0.95 * vs[i][at] + 0.05 * grad * grad
        w = ws[i][at].astype(F32)
        new_ws[i][at] = (w - 0.02 * (m * lax.rsqrt(v + 1e-8) + 0.1 * w)).astype(BF16)
        new_ms[i][at] = m
        new_vs[i][at] = v

    def grad_rows(start):
        return g[0, start : start + BLOCK, :]

    for i in range(2):
        for t in range(d // BLOCK):
            update(i, (0, slice(t * BLOCK, (t + 1) * BLOCK), slice(None)), grad_rows(i * d + t * BLOCK))
    for t in range(d // BLOCK):
        update(2, (0, slice(None), slice(t * BLOCK, (t + 1) * BLOCK)), grad_rows(2 * d + t * BLOCK))


def adamw(factor, g, weights, m, v):
    layers, d, ff = weights[0].shape
    blocks = ff // BLOCK
    tall = pl.BlockSpec((1, d, BLOCK), lambda l, j: (l, 0, j))
    flat = pl.BlockSpec((1, BLOCK, d), lambda l, j: (l, j, 0))
    three = [tall, tall, flat]
    return pl.pallas_call(
        functools.partial(adamw_kernel, 1, d),
        out_shape=[jax.ShapeDtypeStruct(o.shape, o.dtype) for o in (*weights, *m, *v)],
        grid=(layers, blocks),
        in_specs=[pl.BlockSpec(memory_space=pltpu.SMEM), pl.BlockSpec((1, 3 * d, BLOCK), lambda l, j: ((layers - 1 - l) * blocks + j, 0, 0))] + three * 3,
        out_specs=three * 3,
        compiler_params=pltpu.CompilerParams(vmem_limit_bytes=VMEM),
        name="adamw",
    )(factor, g, *weights, *m, *v)


def solution(mesh):
    group = mesh.shape["dp"]

    def step(x, dy, *arrays):
        weights, m, v = (arrays[i : i + 3] for i in (0, 3, 6))
        h1 = forward(x[0], *weights)
        g, squares = backward(group, h1, x[0], dy[0], *weights)
        g = g.reshape(g.shape[0], -1, g.shape[-1])
        factor = jnp.minimum(1.0, 0.5 * lax.rsqrt(squares[0, :1] / g.size + 1e-30))
        return tuple(adamw(factor, g, weights, m, v))

    return jax.shard_map(
        step,
        mesh=mesh,
        in_specs=(P(("rep", "dp"), None, None),) * 2 + (P(None, None, None),) * 9,
        out_specs=(P("rep", None, None),) * 9,
        check_vma=False,
    )
```
